32 devices in a mesh: gx: 8 (over y, x, core), gy: 4 (over z).
Axes of the slice: x: 2, y: 2, z: 4, core: 2. Of those that a mesh axis runs over, the one named last changes fastest.
Arguments:
- candidate_owner: int32 [256, 512, 1], P(('gx', 'gy')), may hold values from 0 to 31; in each aligned block of 4096 rows (0 to 4095, 4096 to 8191, ..., all dimensions but the last counted through in order) at most 256 rows name the same one
- candidate_row: int32 [256, 512], P(('gx', 'gy')), may hold values from 0 to 78335
- item_table: bfloat16 [2506752, 128], P(('gx', 'gy')), may hold values from -6 to 6
- w_in: bfloat16 [128, 512], replicated, may hold values from -0.5 to 0.5
- w_qkv: bfloat16 [1, 512, 1536], replicated, may hold values from -0.25 to 0.25
- w_out: bfloat16 [1, 512, 512], replicated, may hold values from -0.25 to 0.25
- w_up: bfloat16 [1, 512, 1024], replicated, may hold values from -0.25 to 0.25
- w_down: bfloat16 [1, 1024, 512], replicated, may hold values from -0.1875 to 0.1875
- norm_gains: float32 [1, 2, 512], replicated, may hold values from 0.25 to 1.75
- final_gain: float32 [512], replicated, may hold values from 0.25 to 1.75
- w_score: bfloat16 [512], replicated, may hold values from -0.25 to 0.25
Outputs:
- log_probs: float32 [256, 512], P(('gx', 'gy'))
The draws below stay inside these ranges and needn't reach their ends.
Inputs may be any that keep to these rules, and one draw needn't show every extreme that they name: `candidate_owner`: among the candidates of one device's 8 slates no shard is named more than 256 times, a bound that some block reaches.
All inputs are finite; a program needn't handle non-finite values.
Results may differ from the reference program's by a relative error of at most 0.0007.
Values may be sent and summed in bfloat16 or wider, within the bound.
A program may use at most 128 MiB of HBM per device.

```python
import math
import jax
import jax.numpy as jnp
import numpy as np
from jax import lax

SLATE_LEN = 512
SLATES_DEV = 8
SLATES = 256
EMB = 128
ROWS_DEV = 78336
ROWS = 2506752
D = 512
HEADS = 8
FF = 1024
LAYERS = 1
CAP = 256
N_GX = 8
N_GY = 4


def set_ends(values, rng, smallest, largest):
    dims = values.shape
    place = [jax.random.randint(jax.random.fold_in(rng, axis), (), 0, dims[axis]) for axis in range(len(dims))]
    values = values.at[tuple(place)].set(smallest)
    longest = dims.index(max(dims))
    place[longest] = (place[longest] + 1) % dims[longest]
    return values.at[tuple(place)].set(largest)


def shard_levels(stream_key, shape, split, smallest, high):
    level, own = 1.0, jax.random.fold_in(stream_key, 6)
    for position, shards_of in split:
        steps = jnp.exp(jax.random.uniform(jax.random.fold_in(own, position), (shards_of,), jnp.float32, smallest / len(split), high / len(split)))
        level = level * jnp.repeat(steps, shape[position] // shards_of).reshape([-1 if axis == position else 1 for axis in range(len(shape))])
    return level


def wide_ids(key, dims, number_of, slope):
    portions = [min(1 << octave, number_of + 1 - (1 << octave)) * (1 << 20) // math.isqrt((1 << octave) ** slope) + 1 for octave in range((number_of + 1).bit_length()) if 1 << octave <= number_of]
    spread = 1 + sum(portions) // (1 << 30)
    listing = np.cumsum(np.array([max(1, weight // spread) for weight in portions]))
    pick = jax.random.randint(jax.random.fold_in(key, 1), dims, 0, int(listing[len(portions) - 1]))
    start = jnp.left_shift(1, jnp.searchsorted(jnp.asarray(listing, jnp.int32), pick, side="right").astype(jnp.int32))
    grade = start - 1 + jax.random.randint(jax.random.fold_in(key, 4), dims, 0, 1 << 30) % jnp.minimum(start, number_of + 1 - start)
    return jax.random.permutation(jax.random.fold_in(key, 2), number_of)[grade].astype(jnp.int32)


def deal_out(rng, own, number, rows, number_of, top, bound, skew):
    sequence = jax.random.permutation(rng, number_of)
    packed, common = load_shares(number_of, rows * top, bound, skew, True), load_shares(number_of, rows * top, bound, skew, False)
    places = jnp.arange(number_of)

    def named(lengths, turn):
        used = int((lengths > 0).sum())
        fixed = max(1, used // 4)
        moved = fixed + (places - fixed + turn * (used - fixed)) % max(1, number_of - fixed)
        return jnp.zeros((number_of,), jnp.int32).at[sequence[jnp.where(places < fixed, places, moved)]].set(jnp.asarray(lengths, jnp.int32))

    lengths = jnp.where(number % 4 == 0, named(packed, number // 4), named(common, number - number // 4 - 1))
    mixed = jax.random.permutation(jax.random.fold_in(own, 3), number_of)
    source_of, sink = mixed[0:number_of // 2 * 2:2], mixed[1:number_of // 2 * 2:2]
    room = jnp.minimum(lengths[source_of] - 1, bound - lengths[sink]) // 2
    room = jnp.where((source_of == sequence[0]) | (sink == sequence[0]) | (lengths[sink] == 0), 0, jnp.maximum(room, 0))
    moved = jax.random.randint(jax.random.fold_in(own, 4), (number_of // 2,), 0, 1 << 20) % (room + 1)
    lengths = lengths.at[source_of].add(-moved).at[sink].add(moved)
    members = jnp.searchsorted(jnp.cumsum(lengths), jnp.arange(rows * top), side="right").astype(jnp.int32)
    grid = members.reshape(top, rows).T
    grid = grid[jax.random.permutation(jax.random.fold_in(own, 1), rows)]
    turn = jax.random.randint(jax.random.fold_in(own, 2), (rows, 1), 0, top)
    return jnp.take_along_axis(grid, (jnp.arange(top)[None, :] + turn) % top, axis=1)


def load_shares(amount, total, limit, lean, full):
    portions = [(1 << 20) // math.isqrt(standing ** lean) + 1 for standing in range(1, amount + 1)]
    largest = limit if full else min(limit, max(-(-total // amount), total * portions[0] // sum(portions)))
    least = 1 if total - largest >= amount - 1 else 0
    holding, rest = [largest] + [least] * (amount - 1), total - largest - least * (amount - 1)
    while rest > 0:
        free = [i for i in range(1, amount) if holding[i] < largest] or [i for i in range(1, amount) if holding[i] < limit]
        pool, budget = sum([portions[i] for i in free]), rest
        for i in free:
            addition = min(limit - holding[i], max(1, budget * portions[i] // pool), rest)
            holding[i] = holding[i] + addition
            rest = rest - addition
    return np.array(holding)


def normal_values(own_key, extent, scale, most, pieces=(), dtype=jnp.bfloat16):
    factor_of = shard_levels(own_key, extent, pieces, -0.22, 0.18) if pieces else 1.0
    drawn = jax.random.normal(own_key, extent, jnp.float32) * scale * factor_of
    return jnp.minimum(jnp.maximum(drawn, -most), most).astype(dtype)


def setup_inputs(seed: int = 0) -> dict:
    arg_keys = jax.random.split(jax.random.key(seed), 12)
    candidate_owner_keys = jax.random.split(jax.random.fold_in(arg_keys[0], 1), SLATES * SLATE_LEN // (SLATES_DEV * SLATE_LEN))
    candidate_owner_turns = jax.random.permutation(jax.random.fold_in(arg_keys[0], 3), SLATES * SLATE_LEN // (SLATES_DEV * SLATE_LEN))
    candidate_owner = jax.vmap(lambda own, number: deal_out(jax.random.fold_in(arg_keys[0], 2), own, number, SLATES_DEV * SLATE_LEN, N_GX * N_GY, 1, CAP, 2))(candidate_owner_keys, candidate_owner_turns).reshape((SLATES, SLATE_LEN, 1))
    candidate_row = set_ends(wide_ids(arg_keys[1], (SLATES, SLATE_LEN), ROWS_DEV, 2), jax.random.fold_in(arg_keys[1], 3), 0, ROWS_DEV - 1).astype(jnp.int32)
    item_table = normal_values(arg_keys[2], (ROWS, EMB), 1.0, 6.0, ((0, 32),))
    w_in = normal_values(arg_keys[3], (EMB, D), EMB ** -0.5, 0.5)
    w_qkv = normal_values(arg_keys[4], (LAYERS, D, 3 * D), D ** -0.5, 0.25)
    w_out = normal_values(arg_keys[5], (LAYERS, D, D), D ** -0.5, 0.25)
    w_up = normal_values(arg_keys[6], (LAYERS, D, FF), D ** -0.5, 0.25)
    w_down = normal_values(arg_keys[7], (LAYERS, FF, D), FF ** -0.5, 0.1875)
    norm_gains = jnp.clip(1.0 + 0.15 * jax.random.normal(arg_keys[8], (LAYERS, 2, D), jnp.float32), 0.25, 1.75)
    final_gain = jnp.clip(1.0 + 0.15 * jax.random.normal(arg_keys[9], (D,), jnp.float32), 0.25, 1.75)
    w_score = normal_values(arg_keys[10], (D,), D ** -0.5, 0.25)
    return dict(candidate_owner=candidate_owner, candidate_row=candidate_row, item_table=item_table, w_in=w_in, w_qkv=w_qkv, w_out=w_out, w_up=w_up, w_down=w_down, norm_gains=norm_gains, final_gain=final_gain, w_score=w_score)


def layer_norm(values, gain):
    mean = lax.optimization_barrier(jnp.mean(values, axis=-1, keepdims=True))
    centred = values - mean
    variance = lax.optimization_barrier(jnp.mean(centred * centred, axis=-1, keepdims=True))
    return centred * lax.rsqrt(variance + 1e-05) * gain

def score_slates(emb, w_in, w_qkv, w_out, w_up, w_down, norm_gains, final_gain, w_score):
    slates, length, width = emb.shape
    model = w_in.shape[1]
    head_dim = model // HEADS
    resid = jnp.dot(emb.reshape(slates * length, width), w_in, preferred_element_type=jnp.float32)
    for layer in range(LAYERS):
        normed = layer_norm(resid, norm_gains[layer, 0]).astype(jnp.bfloat16)
        qkv = jnp.dot(normed, w_qkv[layer], preferred_element_type=jnp.float32).astype(jnp.bfloat16)
        qkv = qkv.reshape(slates, length, 3, HEADS, head_dim)
        query = qkv[:, :, 0].astype(jnp.float32)
        keys = qkv[:, :, 1].astype(jnp.float32)
        values = qkv[:, :, 2].astype(jnp.float32)
        scores = jnp.einsum('bqhd,bkhd->bhqk', query, keys) * head_dim ** (-0.5)
        probs = jax.nn.softmax(scores, axis=-1).astype(jnp.bfloat16)
        mixed = jnp.einsum('bhqk,bkhd->bqhd', probs.astype(jnp.float32), values)
        mixed = mixed.astype(jnp.bfloat16).reshape(slates * length, model)
        resid = resid + jnp.dot(mixed, w_out[layer], preferred_element_type=jnp.float32)
        normed = layer_norm(resid, norm_gains[layer, 1]).astype(jnp.bfloat16)
        inner = jax.nn.gelu(jnp.dot(normed, w_up[layer], preferred_element_type=jnp.float32)).astype(jnp.bfloat16)
        resid = resid + jnp.dot(inner, w_down[layer], preferred_element_type=jnp.float32)
    final = layer_norm(resid, final_gain)
    logits = lax.optimization_barrier(jnp.sum(final * w_score.astype(jnp.float32)[None, :], axis=-1))
    return jax.nn.log_softmax(logits.reshape(slates, length), axis=-1)

def reference(candidate_owner, candidate_row, item_table, w_in, w_qkv, w_out, w_up, w_down, norm_gains, final_gain, w_score):
    item = (candidate_owner[:, :, 0] * ROWS_DEV + candidate_row).astype(jnp.int32)
    emb = jnp.take(item_table, item.reshape(-1), axis=0)
    emb = emb.reshape(N_GX * N_GY * SLATES_DEV, 1, SLATE_LEN, EMB)

    def one_group(block):
        return score_slates(block, w_in, w_qkv, w_out, w_up, w_down, norm_gains, final_gain, w_score)
    scored = lax.map(one_group, emb)
    return scored.reshape(SLATES, SLATE_LEN)
```

```python
import functools
import jax
import jax.numpy as jnp
from jax import lax
from jax.experimental import pallas as pl
from jax.experimental.pallas import tpu as pltpu
from jax.sharding import PartitionSpec as P

HEADS = 8
PICK = 32
CHUNKS = 2
LOG2E = 1.4426950408889634


def layer_norm(values, gain):
    mean = jnp.mean(values, axis=-1, keepdims=True)
    centred = values - mean
    variance = jnp.mean(centred * centred, axis=-1, keepdims=True)
    return centred * lax.rsqrt(variance + 1e-05) * gain


def slate_kernel(chunks, place_ref, *refs):
    returned_refs = refs[:chunks]
    (
        w_in_ref, w_qkv_ref, w_out_ref, w_up_ref, w_down_ref, gains_ref, fgain_ref, score_ref,
        out_ref, rows_ref, emb_ref,
    ) = refs[chunks:]
    f32, bf16 = jnp.float32, jnp.bfloat16
    slate = pl.program_id(0)

    @pl.when(slate == 0)
    def _():
        for chunk, ref in enumerate(returned_refs):
            size = ref.shape[0]
            rows_ref[chunk * size : (chunk + 1) * size, :] = ref[...].astype(f32)

    base = slate * emb_ref.shape[0]

    def pick(block, carry):
        for row in range(PICK):
            index = block * PICK + row
            emb_ref[pl.ds(index, 1), :] = rows_ref[pl.ds(place_ref[base + index], 1), :]
        return carry

    lax.fori_loop(0, emb_ref.shape[0] // PICK, pick, 0)
    model = w_in_ref.shape[1]
    head_dim = model // HEADS
    length = emb_ref.shape[0]
    pack = 128 // head_dim
    resid = jnp.dot(emb_ref[...].astype(bf16), w_in_ref[...], preferred_element_type=f32)
    normed = layer_norm(resid, gains_ref[0:1, :]).astype(bf16)
    query = jnp.dot(normed, w_qkv_ref[:, :model], preferred_element_type=f32)
    query = (query * (LOG2E * head_dim ** (-0.5))).astype(bf16)
    keys = jnp.dot(normed, w_qkv_ref[:, model : 2 * model], preferred_element_type=f32).astype(bf16)
    values = jnp.dot(normed, w_qkv_ref[:, 2 * model :], preferred_element_type=f32).astype(bf16)
    ones = jnp.ones((length, 128), bf16)
    lane = lax.broadcasted_iota(jnp.int32, (length, 128), 1) // head_dim
    mixed = []
    for group in range(HEADS // pack):
        cols = slice(group * 128, (group + 1) * 128)
        q_g, k_g = query[:, cols], keys[:, cols]
        v_g = jnp.concatenate([values[:, cols], ones], axis=1)
        total = None
        for part in range(pack):
            q_h = jnp.where(lane == part, q_g, jnp.zeros_like(q_g))
            scores = lax.dot_general(q_h, k_g, (((1,), (1,)), ((), ())), preferred_element_type=f32)
            top = jnp.max(scores, axis=-1, keepdims=True)
            probs = jnp.exp2(scores - top).astype(bf16)
            both = jnp.dot(probs, v_g, preferred_element_type=f32)
            head = both[:, :128] / both[:, 128:]
            total = head if total is None else jnp.where(lane == part, head, total)
        mixed.append(total.astype(bf16))
    mixed = jnp.concatenate(mixed, axis=1)
    resid = resid + jnp.dot(mixed, w_out_ref[...], preferred_element_type=f32)
    normed = layer_norm(resid, gains_ref[1:2, :]).astype(bf16)
    inner = jax.nn.gelu(jnp.dot(normed, w_up_ref[...], preferred_element_type=f32)).astype(bf16)
    resid = resid + jnp.dot(inner, w_down_ref[...], preferred_element_type=f32)
    terms = layer_norm(resid, fgain_ref[...]) * score_ref[...]
    folded = terms[:, :128]
    for start in range(128, model, 128):
        folded = folded + terms[:, start : start + 128]
    logits = jnp.sum(folded.T, axis=0, keepdims=True)
    shifted = logits - jnp.max(logits, axis=-1, keepdims=True)
    out_ref[0] = shifted - jnp.log(jnp.sum(jnp.exp(shifted), axis=-1, keepdims=True))


def score_slates(returned, position, w_in, w_qkv, w_out, w_up, w_down, norm_gains, final_gain, w_score):
    slates, length = position.shape
    chunks, width = len(returned), returned[0].shape[1]
    weights = (
        w_in,
        w_qkv[0],
        w_out[0],
        w_up[0],
        w_down[0],
        norm_gains[0],
        final_gain[None, :],
        w_score.astype(jnp.float32)[None, :],
    )
    whole = lambda w: pl.BlockSpec(w.shape, lambda s, place: (0, 0))
    out = pl.pallas_call(
        functools.partial(slate_kernel, chunks),
        grid_spec=pltpu.PrefetchScalarGridSpec(
            num_scalar_prefetch=1,
            grid=(slates,),
            in_specs=[whole(w) for w in (*returned, *weights)],
            out_specs=pl.BlockSpec((1, 1, length), lambda s, place: (s, 0, 0)),
            scratch_shapes=[
                pltpu.VMEM((chunks * returned[0].shape[0], width), jnp.float32),
                pltpu.VMEM((length, width), jnp.float32),
            ],
        ),
        out_shape=jax.ShapeDtypeStruct((slates, 1, length), jnp.float32),
        compiler_params=pltpu.CompilerParams(vmem_limit_bytes=60 * 1024 * 1024),
        name="slates",
    )(position.reshape(-1), *returned, *weights)
    return out.reshape(slates, length)


def slots_and_requests(owner, row_index, shards, capacity, length):
    total = owner.shape[0]
    onehot = (owner[:, None] == jnp.arange(shards, dtype=jnp.int32)[None, :]).astype(jnp.bfloat16)
    blocks = onehot.reshape(total // length, length, shards)
    lower = (jnp.arange(length)[:, None] >= jnp.arange(length)[None, :]).astype(jnp.bfloat16)
    within = jnp.einsum("ij,bjn->bin", lower, blocks, preferred_element_type=jnp.float32)
    totals = within[:, -1, :]
    before = jnp.cumsum(totals, axis=0) - totals
    counts = within + before[:, None, :]
    picked = jnp.sum(counts * blocks.astype(jnp.float32), axis=-1)
    slot = (picked.reshape(total) - 1.0).astype(jnp.int32)
    at_slot = (slot[:, None] == jnp.arange(capacity, dtype=jnp.int32)[None, :]).astype(jnp.bfloat16)
    digits = jnp.stack([row_index >> 16, (row_index >> 8) & 255, row_index & 255], axis=1).astype(jnp.bfloat16)
    placed = (onehot[:, None, :] * digits[:, :, None]).reshape(total, 3 * shards)
    found = lax.dot_general(placed, at_slot, (((0,), (0,)), ((), ())), preferred_element_type=jnp.float32)
    found = found.astype(jnp.int32).reshape(3, shards, capacity)
    return slot, (found[0] << 16) + (found[1] << 8) + found[2]


def exchange_kernel(blocks_ref, out_ref, send_sems, recv_sems, own_sem):
    inner = lax.axis_size("gy")
    count = lax.axis_size("gx") * inner
    here = lax.axis_index("gx") * inner + lax.axis_index("gy")
    barrier = pltpu.get_barrier_semaphore()

    def place(step):
        peer = lax.rem(here + step, count)
        return peer, (peer // inner, lax.rem(peer, inner))

    def copy_of(step):
        peer, device = place(step)
        return pltpu.make_async_remote_copy(
            src_ref=blocks_ref.at[peer],
            dst_ref=out_ref.at[here],
            send_sem=send_sems.at[step],
            recv_sem=recv_sems.at[step],
            device_id=device,
            device_id_type=pl.DeviceIdType.MESH,
        )

    @pl.loop(1, count)
    def _(step):
        pl.semaphore_signal(barrier, inc=1, device_id=place(step)[1], device_id_type=pl.DeviceIdType.MESH)

    own = pltpu.make_async_copy(blocks_ref.at[here], out_ref.at[here], own_sem)
    own.start()
    pl.semaphore_wait(barrier, count - 1)

    @pl.loop(1, count)
    def _(step):
        copy_of(step).start()

    @pl.loop(1, count)
    def _(step):
        copy_of(step).wait()

    own.wait()


def exchange(blocks, collective_id, space):
    count = blocks.shape[0]
    return pl.pallas_call(
        exchange_kernel,
        out_shape=jax.ShapeDtypeStruct(blocks.shape, blocks.dtype),
        in_specs=[pl.BlockSpec(memory_space=space)],
        out_specs=pl.BlockSpec(memory_space=space),
        scratch_shapes=[
            pltpu.SemaphoreType.DMA((count,)),
            pltpu.SemaphoreType.DMA((count,)),
            pltpu.SemaphoreType.DMA,
        ],
        compiler_params=pltpu.CompilerParams(
            collective_id=collective_id, has_side_effects=True, vmem_limit_bytes=32 * 1024 * 1024
        ),
        name="exchange",
    )(blocks)


def pick_kernel(asked_ref, table_ref, out_ref, rows_ref, stage_ref):
    step, steps = pl.program_id(0), pl.num_programs(0)
    size = table_ref.shape[0]
    start = pl.multiple_of(step * size, size)
    rows_ref[pl.ds(start, size), :] = table_ref[...].astype(jnp.float32)

    @pl.when(step == steps - 1)
    def _():
        def pick(block, carry):
            for row in range(PICK):
                index = block * PICK + row
                stage_ref[pl.ds(index, 1), :] = rows_ref[pl.ds(asked_ref[index], 1), :]
            return carry

        lax.fori_loop(0, out_ref.shape[0] // PICK, pick, 0)
        out_ref[...] = stage_ref[...].astype(out_ref.dtype)


def pick_rows(item_table, asked):
    rows, width = item_table.shape
    count = asked.shape[0]
    size = next(size for size in range(4608, 0, -16) if rows % size == 0)
    return pl.pallas_call(
        pick_kernel,
        grid_spec=pltpu.PrefetchScalarGridSpec(
            num_scalar_prefetch=1,
            grid=(rows // size,),
            in_specs=[pl.BlockSpec((size, width), lambda s, asked: (s, 0))],
            out_specs=pl.BlockSpec((count, width), lambda s, asked: (0, 0)),
            scratch_shapes=[pltpu.VMEM((rows, width), jnp.float32), pltpu.VMEM((count, width), jnp.float32)],
        ),
        out_shape=jax.ShapeDtypeStruct((count, width), item_table.dtype),
        compiler_params=pltpu.CompilerParams(vmem_limit_bytes=60 * 1024 * 1024),
        name="pick_rows",
    )(asked, item_table)


def per_device(
    candidate_owner,
    candidate_row,
    item_table,
    w_in,
    w_qkv,
    w_out,
    w_up,
    w_down,
    norm_gains,
    final_gain,
    w_score,
):
    slates, length, unused = candidate_owner.shape
    width = item_table.shape[1]
    shards = lax.axis_size(("gx", "gy"))
    capacity = max(2, 2 * slates * length // shards)
    owner = candidate_owner.reshape(slates * length)
    row_index = candidate_row.reshape(slates * length)
    slot, outgoing = slots_and_requests(owner, row_index, shards, capacity, length)
    wanted = exchange(outgoing[:, None, :], 0, pltpu.VMEM).reshape(shards, capacity)
    chunks = CHUNKS if capacity % CHUNKS == 0 else 1
    depth = capacity // chunks
    returned = []
    for chunk in range(chunks):
        asked = wanted[:, chunk * depth : (chunk + 1) * depth].reshape(-1)
        found = pick_rows(item_table, asked).reshape(shards, depth, width)
        back = lax.all_to_all(found, ("gx", "gy"), split_axis=0, concat_axis=0, tiled=True)
        returned.append(back.reshape(shards * depth, width))
    position = (slot // depth) * (shards * depth) + owner * depth + slot % depth
    position = position.reshape(slates, length)
    return score_slates(
        returned, position, w_in, w_qkv, w_out, w_up, w_down, norm_gains, final_gain, w_score
    )


def solution(mesh):
    return jax.shard_map(
        per_device,
        mesh=mesh,
        in_specs=(
            P(("gx", "gy"), None, None),
            P(("gx", "gy"), None),
            P(("gx", "gy"), None),
            P(),
            P(),
            P(),
            P(),
            P(),
            P(),
            P(),
            P(),
        ),
        out_specs=P(("gx", "gy"), None),
        check_vma=False,
    )
```
